64 devices in a mesh: dp: 8 (over x, y, core), tp: 8 (over z).
Axes of the slice: x: 2, y: 2, z: 8, core: 2. Of those that a mesh axis runs over, the one named last changes fastest.
The devices are a block of a 4x4x8 slice.
Arguments:
- x: bfloat16 [16384, 3072], P('dp'), parts along dimension 0
- w_gate: bfloat16 [3072, 24576], P(None, 'tp')
- w_up: bfloat16 [3072, 24576], P(None, 'tp')
- w_down: bfloat16 [24576, 3072], P('tp')
Outputs:
- output: bfloat16 [16384, 3072], P('dp'), parts along dimension 0
There are 8 independent parts. The reference program is written for one: setup_inputs(seed, part) draws one part's arguments, and reference() takes and returns one part's arrays. A program takes and returns all parts, laid end to end along the dimension named above; an argument that names none is the same for every part.
All inputs are finite; a program needn't handle non-finite values.
Results may differ from the reference program's by a relative error of at most 0.016.
Values are sent between devices in bfloat16 or wider.
A program may use at most 768 MiB of HBM per device.

```python
import jax
import jax.numpy as jnp

ROWS = 2048
D = 3072
FF = 24576


def setup_inputs(seed: int = 0, part: int = 0) -> dict:
    kx, kg, ku, kd = jax.random.split(jax.random.key(seed), 4)
    drawn = {
        "x": jax.random.normal(jax.random.fold_in(kx, part), (ROWS, D), jnp.float32),
        "w_gate": jax.random.normal(kg, (D, FF), jnp.float32) * D**-0.5,
        "w_up": jax.random.normal(ku, (D, FF), jnp.float32) * D**-0.5,
        "w_down": jax.random.normal(kd, (FF, D), jnp.float32) * FF**-0.5,
    }
    return {k: v.astype(jnp.bfloat16) for k, v in drawn.items()}


def reference(x, w_gate, w_up, w_down):
    gate = jnp.dot(x, w_gate, preferred_element_type=jnp.float32)
    up = jnp.dot(x, w_up, preferred_element_type=jnp.float32)
    hidden = (jax.nn.gelu(gate) * up).astype(jnp.bfloat16)
    return jnp.dot(hidden, w_down, preferred_element_type=jnp.float32).astype(jnp.bfloat16)
```

```python
import functools
import math

import jax
import jax.numpy as jnp
from jax import lax
from jax.experimental import pallas as pl
from jax.experimental.pallas import tpu as pltpu
from jax.sharding import PartitionSpec as P

MESH = pl.DeviceIdType.MESH
TILE = 512
SLOTS = 3


def gelu(v):
    c = math.sqrt(2.0 / math.pi)
    return (0.5 * v) * (1.0 + jnp.tanh(v * (c + (c * 0.044715) * (v * v))))


def kernel(
    n, x_ref, wg_hbm, wu_hbm, wd_hbm, y_ref, wg, wu, wd, xb, hb, x_sem, w_sem, d_sem, send_sem, recv_sem
):
    rows, depth = x_ref.shape
    width = wg_hbm.shape[1]
    out = wd_hbm.shape[1]
    block = rows // n
    half = block // 2
    nt = width // TILE
    ct = out // TILE
    me = lax.axis_index("tp")
    right, left = lax.rem(me + 1, n), lax.rem(me + n - 1, n)

    barrier = pltpu.get_barrier_semaphore()
    for neighbour in (left, right):
        pl.semaphore_signal(barrier, inc=1, device_id={"tp": neighbour}, device_id_type=MESH)

    def rows_a(s):
        return pl.ds(pl.multiple_of(lax.rem(me + 2 * n - s, n) * block, block), half)

    def rows_b(s):
        return pl.ds(pl.multiple_of(lax.rem(me + s, n) * block + half, half), half)

    def cols(t):
        return pl.ds(pl.multiple_of(t * TILE, TILE), TILE)

    def x_copies(s):
        return (
            pltpu.make_async_copy(x_ref.at[rows_a(s)], xb.at[pl.ds(0, half)], x_sem.at[0]),
            pltpu.make_async_copy(x_ref.at[rows_b(s)], xb.at[pl.ds(half, half)], x_sem.at[1]),
        )

    def w_copies(t):
        return (
            pltpu.make_async_copy(wg_hbm.at[:, cols(t)], wg.at[t], w_sem.at[0, t]),
            pltpu.make_async_copy(wu_hbm.at[:, cols(t)], wu.at[t], w_sem.at[1, t]),
        )

    def d_copy(q):
        slot = lax.rem(q, SLOTS)
        return pltpu.make_async_copy(wd_hbm.at[:, cols(lax.rem(q, ct))], wd.at[slot], d_sem.at[slot])

    def hop(s, t):
        p = lax.rem(s, 2)
        pair = []
        for d, (at, to) in enumerate(((rows_a(s), right), (rows_b(s), left))):
            ref = y_ref.at[at, cols(t)]
            pair.append(
                pltpu.make_async_remote_copy(
                    src_ref=ref,
                    dst_ref=ref,
                    send_sem=send_sem.at[d, p, t],
                    recv_sem=recv_sem.at[d, p, t],
                    device_id={"tp": to},
                    device_id_type=MESH,
                )
            )
        return pair

    def arrived(s, t):
        p = lax.rem(s, 2)
        for d, at in enumerate((rows_a(s + 1), rows_b(s + 1))):
            ref = y_ref.at[at, cols(t)]
            pltpu.make_async_remote_copy(
                src_ref=ref,
                dst_ref=ref,
                send_sem=send_sem.at[d, p, t],
                recv_sem=recv_sem.at[d, p, t],
                device_id={"tp": right},
                device_id_type=MESH,
            ).wait_recv()

    def sent(s, t):
        for copy in hop(s, t):
            copy.wait_send()

    def gate_up(t, first):
        if first:
            for copy in w_copies(t):
                copy.wait()

            @pl.when(t + 2 < nt)
            def _():
                for copy in w_copies(t + 2):
                    copy.start()

            @pl.when(t + 2 >= nt)
            def _():
                d_copy(t + 2 - nt).start()

        gate = jnp.dot(xb[...], wg[t], preferred_element_type=jnp.float32)
        up = jnp.dot(xb[...], wu[t], preferred_element_type=jnp.float32)
        hb[:, cols(t)] = (gelu(gate) * up).astype(hb.dtype)

    def down(s, t, first):
        q = s * ct + t
        d_copy(q).wait()
        term = jnp.dot(hb[...], wd[lax.rem(q, SLOTS)], preferred_element_type=jnp.float32)

        @pl.when(q + SLOTS < n * ct)
        def _():
            d_copy(q + SLOTS).start()

        upper, lower = term[:half], term[half:]
        if not first:
            arrived(s - 1, t)
            upper += y_ref[rows_a(s), cols(t)].astype(jnp.float32)
            lower += y_ref[rows_b(s), cols(t)].astype(jnp.float32)
        y_ref[rows_a(s), cols(t)] = upper.astype(y_ref.dtype)
        y_ref[rows_b(s), cols(t)] = lower.astype(y_ref.dtype)
        if not first:

            @pl.when(s >= 2)
            def _():
                sent(s - 2, t)

        for copy in hop(s, t):
            copy.start()

    def step(s, first):
        for copy in x_copies(s):
            copy.wait()
        pl.loop(0, nt)(lambda t: gate_up(t, first))

        @pl.when(s + 1 < n)
        def _():
            for copy in x_copies(s + 1):
                copy.start()

        if first:
            for t in range(2, SLOTS):
                d_copy(t).start()
            pl.semaphore_wait(barrier, 2)
        pl.loop(0, ct)(lambda t: down(s, t, first))

    for copy in x_copies(0):
        copy.start()
    for t in range(2):
        for copy in w_copies(t):
            copy.start()
    step(0, True)
    pl.loop(1, n)(lambda s: step(s, False))

    @pl.loop(n, 2 * n - 2)
    def _(s):
        @pl.loop(0, ct)
        def _(t):
            arrived(s - 1, t)
            sent(s - 2, t)
            for copy in hop(s, t):
                copy.start()

    @pl.loop(0, ct)
    def _(t):
        arrived(2 * n - 3, t)
        sent(2 * n - 4, t)
        sent(2 * n - 3, t)


def copy_out(parts, v_ref, o_ref, sem):
    size = v_ref.shape[0] // parts
    copies = [
        pltpu.make_async_copy(v_ref.at[pl.ds(k * size, size)], o_ref.at[pl.ds(k * size, size)], sem.at[k])
        for k in range(parts)
    ]
    for copy in copies:
        copy.start()
    for copy in copies:
        copy.wait()


def solution(mesh):
    n = mesh.shape["tp"]

    def step(x, w_gate, w_up, w_down):
        rows, depth = x.shape
        width, out = w_down.shape
        block = rows // n
        y = pl.pallas_call(
            functools.partial(kernel, n),
            out_shape=pltpu.VMEM((rows, out), x.dtype),
            in_specs=[pl.BlockSpec(memory_space=pl.ANY)] * 4,
            out_specs=pl.BlockSpec(memory_space=pltpu.VMEM),
            scratch_shapes=[
                pltpu.VMEM((width // TILE, depth, TILE), x.dtype),
                pltpu.VMEM((width // TILE, depth, TILE), x.dtype),
                pltpu.VMEM((SLOTS, width, TILE), x.dtype),
                pltpu.VMEM((block, depth), x.dtype),
                pltpu.VMEM((block, width), x.dtype),
                pltpu.SemaphoreType.DMA((2,)),
                pltpu.SemaphoreType.DMA((2, width // TILE)),
                pltpu.SemaphoreType.DMA((SLOTS,)),
                pltpu.SemaphoreType.DMA((2, 2, out // TILE)),
                pltpu.SemaphoreType.DMA((2, 2, out // TILE)),
            ],
            compiler_params=pltpu.CompilerParams(
                collective_id=0, has_side_effects=True, vmem_limit_bytes=67043328 - rows * out * 2
            ),
        )(x, w_gate, w_up, w_down)
        return pl.pallas_call(
            functools.partial(copy_out, n),
            out_shape=jax.ShapeDtypeStruct(y.shape, y.dtype),
            in_specs=[pl.BlockSpec(memory_space=pltpu.VMEM)],
            out_specs=pl.BlockSpec(memory_space=pl.ANY),
            scratch_shapes=[pltpu.SemaphoreType.DMA((n,))],
            compiler_params=pltpu.CompilerParams(vmem_limit_bytes=1 << 20),
        )(y)

    return jax.shard_map(
        step,
        mesh=mesh,
        in_specs=(P("dp", None), P(None, "tp"), P(None, "tp"), P("tp", None)),
        out_specs=P("dp", None),
        check_vma=False,
    )
```

```python
import functools
import math

import jax
import jax.numpy as jnp
from jax import lax
from jax.experimental import pallas as pl
from jax.experimental.pallas import tpu as pltpu
from jax.sharding import PartitionSpec as P

MESH = pl.DeviceIdType.MESH
TILE = 512
SLOTS = 2


def gelu(v):
    c = math.sqrt(2.0 / math.pi)
    return (0.5 * v) * (1.0 + jnp.tanh(v * (c + (c * 0.044715) * (v * v))))


def kernel(
    n, x_ref, wg_hbm, wu_hbm, wd_hbm, y_ref, wg, wu, wd, xb, hb, x_sem, w_sem, d_sem, send_sem, recv_sem
):
    rows, depth = x_ref.shape
    width = wg_hbm.shape[1]
    out = wd_hbm.shape[1]
    block = rows // n
    half = block // 2
    nt = width // TILE
    ct = out // TILE
    me = lax.axis_index("tp")
    right, left = lax.rem(me + 1, n), lax.rem(me + n - 1, n)

    barrier = pltpu.get_barrier_semaphore()
    for neighbour in (left, right):
        pl.semaphore_signal(barrier, inc=1, device_id={"tp": neighbour}, device_id_type=MESH)

    def rows_a(s):
        return pl.ds(pl.multiple_of(lax.rem(me + 2 * n - s, n) * block, block), half)

    def rows_b(s):
        return pl.ds(pl.multiple_of(lax.rem(me + s, n) * block + half, half), half)

    def cols(t):
        return pl.ds(pl.multiple_of(t * TILE, TILE), TILE)

    def x_copies(s):
        p = lax.rem(s, 2)
        return (
            pltpu.make_async_copy(x_ref.at[rows_a(s)], xb.at[p, pl.ds(0, half)], x_sem.at[p, 0]),
            pltpu.make_async_copy(x_ref.at[rows_b(s)], xb.at[p, pl.ds(half, half)], x_sem.at[p, 1]),
        )

    def w_copies(t):
        return (
            pltpu.make_async_copy(wg_hbm.at[:, cols(t)], wg.at[t], w_sem.at[0, t]),
            pltpu.make_async_copy(wu_hbm.at[:, cols(t)], wu.at[t], w_sem.at[1, t]),
        )

    def d_copy(q):
        slot = lax.rem(q, SLOTS)
        return pltpu.make_async_copy(wd_hbm.at[:, cols(lax.rem(q, ct))], wd.at[slot], d_sem.at[slot])

    def hop(s, t):
        p = lax.rem(s, 2)
        pair = []
        for d, (at, to) in enumerate(((rows_a(s), right), (rows_b(s), left))):
            ref = y_ref.at[at, cols(t)]
            pair.append(
                pltpu.make_async_remote_copy(
                    src_ref=ref,
                    dst_ref=ref,
                    send_sem=send_sem.at[d, t],
                    recv_sem=recv_sem.at[d, p, t],
                    device_id={"tp": to},
                    device_id_type=MESH,
                )
            )
        return pair

    def arrived(s, t):
        p = lax.rem(s, 2)
        for d, at in enumerate((rows_a(s + 1), rows_b(s + 1))):
            ref = y_ref.at[at, cols(t)]
            pltpu.make_async_remote_copy(
                src_ref=ref,
                dst_ref=ref,
                send_sem=send_sem.at[d, t],
                recv_sem=recv_sem.at[d, p, t],
                device_id={"tp": right},
                device_id_type=MESH,
            ).wait_recv()

    def sent(s, t):
        for copy in hop(s, t):
            copy.wait_send()

    def gate_up(s, t):
        p = lax.rem(s, 2)
        gate = jnp.dot(xb[p], wg[t], preferred_element_type=jnp.float32)
        up = jnp.dot(xb[p], wu[t], preferred_element_type=jnp.float32)
        hb[p, :, cols(t)] = (gelu(gate) * up).astype(hb.dtype)

    def down(s, t, first=False):
        slot = lax.rem(s * ct + t, SLOTS)
        for k, at in enumerate((rows_a(s), rows_b(s))):
            part = jnp.dot(hb[lax.rem(s, 2), pl.ds(k * half, half)], wd[slot], preferred_element_type=jnp.float32)
            if not first:
                part += y_ref[at, cols(t)].astype(jnp.float32)
            y_ref[at, cols(t)] = part.astype(y_ref.dtype)

    def ready(s, t):
        d_copy(s * ct + t).wait()
        arrived(s - 1, t)
        sent(s - 1, t)

    def send(s, t):
        for copy in hop(s, t):
            copy.start()

    def begin(s):
        for copy in x_copies(s + 1):
            copy.wait()

        @pl.when(s + 2 < n)
        def _():
            for copy in x_copies(s + 2):
                copy.start()

    for copy in x_copies(0):
        copy.start()
    for copy in w_copies(0):
        copy.start()
    for copy in x_copies(0):
        copy.wait()
    for copy in w_copies(1):
        copy.start()

    @pl.loop(0, nt)
    def _(t):
        for copy in w_copies(t):
            copy.wait()

        @pl.when(t + 2 < nt)
        def _():
            for copy in w_copies(t + 2):
                copy.start()

        @pl.when(t + 2 == nt)
        def _():
            d_copy(0).start()

        @pl.when(t + 1 == nt)
        def _():
            for copy in x_copies(1):
                copy.start()
            for q in range(1, SLOTS):
                d_copy(q).start()

        gate_up(0, t)

    pl.semaphore_wait(barrier, 2)

    def down_alone(s, t):
        ready(s, t)
        down(s, t)
        send(s, t)
        d_copy(s * ct + t + SLOTS).start()

    @pl.loop(0, ct)
    def _(t):
        d_copy(t).wait()
        down(0, t, True)
        send(0, t)
        d_copy(t + SLOTS).start()

        @pl.when(t == 0)
        def _():
            begin(0)

        gate_up(1, t)

    down_alone(1, 0)

    @pl.loop(1, n - 1)
    def _(s):
        begin(s)

        @pl.loop(1, ct)
        def _(t):
            ready(s, t)
            down(s, t)
            gate_up(s + 1, t - 1)
            send(s, t)
            d_copy(s * ct + t + SLOTS).start()

        gate_up(s + 1, nt - 1)
        down_alone(s + 1, 0)

    pl.loop(1, ct)(lambda t: down_alone(n - 1, t))
    for t in range(SLOTS):
        d_copy(n * ct + t).wait()

    @pl.loop(n, 2 * n - 2)
    def _(s):
        @pl.loop(0, ct)
        def _(t):
            arrived(s - 1, t)
            sent(s - 1, t)
            for copy in hop(s, t):
                copy.start()

    @pl.loop(0, ct)
    def _(t):
        arrived(2 * n - 3, t)
        sent(2 * n - 3, t)


def copy_out(parts, v_ref, o_ref, sem):
    size = v_ref.shape[0] // parts
    copies = [
        pltpu.make_async_copy(v_ref.at[pl.ds(k * size, size)], o_ref.at[pl.ds(k * size, size)], sem.at[k])
        for k in range(parts)
    ]
    for copy in copies:
        copy.start()
    for copy in copies:
        copy.wait()


def solution(mesh):
    n = mesh.shape["tp"]

    def step(x, w_gate, w_up, w_down):
        rows, depth = x.shape
        width, out = w_down.shape
        block = rows // n
        y = pl.pallas_call(
            functools.partial(kernel, n),
            out_shape=pltpu.VMEM((rows, out), x.dtype),
            in_specs=[pl.BlockSpec(memory_space=pl.ANY)] * 4,
            out_specs=pl.BlockSpec(memory_space=pltpu.VMEM),
            scratch_shapes=[
                pltpu.VMEM((width // TILE, depth, TILE), x.dtype),
                pltpu.VMEM((width // TILE, depth, TILE), x.dtype),
                pltpu.VMEM((SLOTS, width, TILE), x.dtype),
                pltpu.VMEM((2, block, depth), x.dtype),
                pltpu.VMEM((2, block, width), x.dtype),
                pltpu.SemaphoreType.DMA((2, 2)),
                pltpu.SemaphoreType.DMA((2, width // TILE)),
                pltpu.SemaphoreType.DMA((SLOTS,)),
                pltpu.SemaphoreType.DMA((2, out // TILE)),
                pltpu.SemaphoreType.DMA((2, 2, out // TILE)),
            ],
            compiler_params=pltpu.CompilerParams(
                collective_id=0, has_side_effects=True, vmem_limit_bytes=67043328 - rows * out * 2
            ),
        )(x, w_gate, w_up, w_down)
        return pl.pallas_call(
            functools.partial(copy_out, n),
            out_shape=jax.ShapeDtypeStruct(y.shape, y.dtype),
            in_specs=[pl.BlockSpec(memory_space=pltpu.VMEM)],
            out_specs=pl.BlockSpec(memory_space=pl.ANY),
            scratch_shapes=[pltpu.SemaphoreType.DMA((n,))],
            compiler_params=pltpu.CompilerParams(vmem_limit_bytes=1 << 20),
        )(y)

    return jax.shard_map(
        step,
        mesh=mesh,
        in_specs=(P("dp", None), P(None, "tp"), P(None, "tp"), P("tp", None)),
        out_specs=P("dp", None),
        check_vma=False,
    )
```

```python
import functools
import math

import jax
import jax.numpy as jnp
from jax import lax
from jax.experimental import pallas as pl
from jax.experimental.pallas import tpu as pltpu
from jax.sharding import PartitionSpec as P

MESH = pl.DeviceIdType.MESH
TILE = 512
SLOTS = 2


def gelu(v):
    c = math.sqrt(2.0 / math.pi)
    return (0.5 * v) * (1.0 + jnp.tanh(v * (c + (c * 0.044715) * (v * v))))


def kernel(
    n, x_ref, wg_hbm, wu_hbm, wd_hbm, y_ref, wg, wu, wd, xb, hb, x_sem, w_sem, d_sem, send_sem, recv_sem
):
    rows, depth = x_ref.shape
    width = wg_hbm.shape[1]
    out = wd_hbm.shape[1]
    block = rows // n
    half = block // 2
    nt = width // TILE
    ct = out // TILE
    me = lax.axis_index("tp")
    right, left = lax.rem(me + 1, n), lax.rem(me + n - 1, n)

    barrier = pltpu.get_barrier_semaphore()
    for neighbour in (left, right):
        pl.semaphore_signal(barrier, inc=1, device_id={"tp": neighbour}, device_id_type=MESH)

    def rows_a(s):
        return pl.ds(pl.multiple_of(lax.rem(me + 2 * n - s, n) * block, block), half)

    def rows_b(s):
        return pl.ds(pl.multiple_of(lax.rem(me + s, n) * block + half, half), half)

    def cols(t):
        return pl.ds(pl.multiple_of(t * TILE, TILE), TILE)

    def x_copies(s):
        p = lax.rem(s, 2)
        return (
            pltpu.make_async_copy(x_ref.at[rows_a(s)], xb.at[p, pl.ds(0, half)], x_sem.at[p, 0]),
            pltpu.make_async_copy(x_ref.at[rows_b(s)], xb.at[p, pl.ds(half, half)], x_sem.at[p, 1]),
        )

    def w_copies(t):
        return (
            pltpu.make_async_copy(wg_hbm.at[:, cols(t)], wg.at[t], w_sem.at[0, t]),
            pltpu.make_async_copy(wu_hbm.at[:, cols(t)], wu.at[t], w_sem.at[1, t]),
        )

    def d_copy(q):
        slot = lax.rem(q, SLOTS)
        return pltpu.make_async_copy(wd_hbm.at[:, cols(lax.rem(q, ct))], wd.at[slot], d_sem.at[slot])

    def hop(s, t):
        p = lax.rem(s, 2)
        pair = []
        for d, (at, to) in enumerate(((rows_a(s), right), (rows_b(s), left))):
            ref = y_ref.at[at, cols(t)]
            pair.append(
                pltpu.make_async_remote_copy(
                    src_ref=ref,
                    dst_ref=ref,
                    send_sem=send_sem.at[d, t],
                    recv_sem=recv_sem.at[d, p, t],
                    device_id={"tp": to},
                    device_id_type=MESH,
                )
            )
        return pair

    def arrived(s, t):
        p = lax.rem(s, 2)
        for d, at in enumerate((rows_a(s + 1), rows_b(s + 1))):
            ref = y_ref.at[at, cols(t)]
            pltpu.make_async_remote_copy(
                src_ref=ref,
                dst_ref=ref,
                send_sem=send_sem.at[d, t],
                recv_sem=recv_sem.at[d, p, t],
                device_id={"tp": right},
                device_id_type=MESH,
            ).wait_recv()

    def sent(s, t):
        for copy in hop(s, t):
            copy.wait_send()

    def gate_up(s, t):
        p = lax.rem(s, 2)
        gate = jnp.dot(xb[p], wg[t], preferred_element_type=jnp.float32)
        up = jnp.dot(xb[p], wu[t], preferred_element_type=jnp.float32)
        hb[p, :, cols(t)] = (gelu(gate) * up).astype(hb.dtype)

    def down(s, t, first=False):
        slot = lax.rem(s * ct + t, SLOTS)
        for k, at in enumerate((rows_a(s), rows_b(s))):
            part = jnp.dot(hb[lax.rem(s, 2), pl.ds(k * half, half)], wd[slot], preferred_element_type=jnp.float32)
            if not first:
                part += y_ref[at, cols(t)].astype(jnp.float32)
            y_ref[at, cols(t)] = part.astype(y_ref.dtype)

    def ready(s, t):
        d_copy(s * ct + t).wait()
        arrived(s - 1, t)

    def send(s, t, first=False):
        if not first:
            sent(s - 1, t)
        for copy in hop(s, t):
            copy.start()

    def begin(s):
        for copy in x_copies(s + 1):
            copy.wait()

        @pl.when(s + 2 < n)
        def _():
            for copy in x_copies(s + 2):
                copy.start()

    for copy in x_copies(0):
        copy.start()
    for copy in w_copies(0):
        copy.start()
    for copy in x_copies(0):
        copy.wait()
    for copy in w_copies(1):
        copy.start()

    @pl.loop(0, nt)
    def _(t):
        for copy in w_copies(t):
            copy.wait()

        @pl.when(t + 2 < nt)
        def _():
            for copy in w_copies(t + 2):
                copy.start()

        @pl.when(t + 2 == nt)
        def _():
            d_copy(0).start()

        @pl.when(t + 1 == nt)
        def _():
            for copy in x_copies(1):
                copy.start()
            for q in range(1, SLOTS):
                d_copy(q).start()

        gate_up(0, t)

    pl.semaphore_wait(barrier, 2)

    def down_alone(s, t):
        ready(s, t)
        down(s, t)
        send(s, t)
        d_copy(s * ct + t + SLOTS).start()

    @pl.loop(0, ct)
    def _(t):
        d_copy(t).wait()
        down(0, t, True)
        send(0, t, True)
        d_copy(t + SLOTS).start()

        @pl.when(t == 0)
        def _():
            begin(0)

        gate_up(1, t)

    down_alone(1, 0)

    @pl.loop(1, n - 1)
    def _(s):
        begin(s)

        @pl.loop(1, ct)
        def _(t):
            ready(s, t)
            down(s, t)
            gate_up(s + 1, t - 1)
            send(s, t)
            d_copy(s * ct + t + SLOTS).start()

        gate_up(s + 1, nt - 1)
        down_alone(s + 1, 0)

    pl.loop(1, ct)(lambda t: down_alone(n - 1, t))
    for t in range(SLOTS):
        d_copy(n * ct + t).wait()

    @pl.loop(n, 2 * n - 2)
    def _(s):
        @pl.loop(0, ct)
        def _(t):
            arrived(s - 1, t)
            sent(s - 1, t)
            for copy in hop(s, t):
                copy.start()

    @pl.loop(0, ct)
    def _(t):
        arrived(2 * n - 3, t)
        sent(2 * n - 3, t)


def copy_out(parts, v_ref, o_ref, sem):
    size = v_ref.shape[0] // parts
    copies = [
        pltpu.make_async_copy(v_ref.at[pl.ds(k * size, size)], o_ref.at[pl.ds(k * size, size)], sem.at[k])
        for k in range(parts)
    ]
    for copy in copies:
        copy.start()
    for copy in copies:
        copy.wait()


def solution(mesh):
    n = mesh.shape["tp"]

    def step(x, w_gate, w_up, w_down):
        rows, depth = x.shape
        width, out = w_down.shape
        block = rows // n
        y = pl.pallas_call(
            functools.partial(kernel, n),
            out_shape=pltpu.VMEM((rows, out), x.dtype),
            in_specs=[pl.BlockSpec(memory_space=pl.ANY)] * 4,
            out_specs=pl.BlockSpec(memory_space=pltpu.VMEM),
            scratch_shapes=[
                pltpu.VMEM((width // TILE, depth, TILE), x.dtype),
                pltpu.VMEM((width // TILE, depth, TILE), x.dtype),
                pltpu.VMEM((SLOTS, width, TILE), x.dtype),
                pltpu.VMEM((2, block, depth), x.dtype),
                pltpu.VMEM((2, block, width), x.dtype),
                pltpu.SemaphoreType.DMA((2, 2)),
                pltpu.SemaphoreType.DMA((2, width // TILE)),
                pltpu.SemaphoreType.DMA((SLOTS,)),
                pltpu.SemaphoreType.DMA((2, out // TILE)),
                pltpu.SemaphoreType.DMA((2, 2, out // TILE)),
            ],
            compiler_params=pltpu.CompilerParams(
                collective_id=0, has_side_effects=True, vmem_limit_bytes=67043328 - rows * out * 2
            ),
        )(x, w_gate, w_up, w_down)
        return pl.pallas_call(
            functools.partial(copy_out, n),
            out_shape=jax.ShapeDtypeStruct(y.shape, y.dtype),
            in_specs=[pl.BlockSpec(memory_space=pltpu.VMEM)],
            out_specs=pl.BlockSpec(memory_space=pl.ANY),
            scratch_shapes=[pltpu.SemaphoreType.DMA((n,))],
            compiler_params=pltpu.CompilerParams(vmem_limit_bytes=1 << 20),
        )(y)

    return jax.shard_map(
        step,
        mesh=mesh,
        in_specs=(P("dp", None), P(None, "tp"), P(None, "tp"), P("tp", None)),
        out_specs=P("dp", None),
        check_vma=False,
    )
```
